128 devices in a mesh: group: 8 (over y_hi, z), shard: 16 (over x, y_lo, core).
Axes of the slice: x: 4, y: 4 (y_hi: 2, y_lo: 2; y = y_hi * 2 + y_lo), z: 4, core: 2. Of those that a mesh axis runs over, the one named last changes fastest.
Arguments:
- hidden_state: bfloat16 [2048, 8192], P('group', 'shard'), may hold values from -40 to 40
- attn_gain: bfloat16 [8192], replicated, may hold values from 0.5 to 1.5
- ffn_gain: bfloat16 [8192], replicated, may hold values from 0.5 to 1.5
- w_query: bfloat16 [8192, 8192], P('group', 'shard'), may hold values from -0.125 to 0.125
- w_keyval: bfloat16 [8192, 2048], P('group', 'shard'), may hold values from -0.0625 to 0.0625
- w_output: bfloat16 [8192, 8192], P('shard', 'group'), may hold values from -0.0625 to 0.0625
- cache_keys: bfloat16 [2048, 8, 192, 128], P(('group', 'shard')), may hold values from -256 to 256
- cache_values: bfloat16 [2048, 8, 192, 128], P(('group', 'shard')), may hold values from -6 to 6
- lengths: int32 [2048], P('group'), may hold values from 2 to 192, as said below
Outputs:
- branch: bfloat16 [2048, 8192], P('group', 'shard')
- ffn_input: bfloat16 [2048, 8192], P('group', 'shard')
The draws below stay inside these ranges and needn't reach their ends.
Inputs may be any that keep to these rules, and one draw needn't show every extreme that they name: `lengths`: in every aligned block of 16 sequences, at least one has all 192 cached positions live.
All inputs are finite; a program needn't handle non-finite values.
Results may differ from the reference program's by a relative error of at most 0.012.
The reference program's roundings to bfloat16 on the way count: a program that leaves them out, or rounds other values in their place, can miss the bound.
Values may be sent and summed in bfloat16 or wider, within the bound.
No kernel may reach another device: no remote copies, remote signals or barrier semaphores. Data moves between devices by JAX's collectives and lax.ppermute only.
A program may use at most 128 MiB of HBM per device.

```python
import jax
import jax.numpy as jnp
from jax import lax

D = 8192
HEADS = 64
KVH = 8
HD = 128
SEQ_DEV = 16
CACHE = 192
SEQS = 2048


def draw_hidden_state(key, part):
    rows_key, cols_key, noise_key = jax.random.split(key, 3)
    position = jnp.arange(D, dtype=jnp.float32) / D
    column_scale = 0.3 * 10.0 ** (0.5 * position + 0.5 * jax.random.uniform(cols_key, (D,), dtype=jnp.float32))
    row_scale = 10.0 ** jax.random.uniform(rows_key, (SEQS, 1), dtype=jnp.float32, minval=-0.5, maxval=0.5)
    values = jax.random.normal(noise_key, (SEQS, D), dtype=jnp.float32) * column_scale[None, :] * row_scale
    return jnp.clip(values, -40.0, 40.0).astype(jnp.bfloat16)


def draw_cache_keys(key, part):
    base_key = jax.random.fold_in(jax.random.fold_in(key, 17), 0)
    shape = (SEQS, KVH, CACHE, HD)
    values = jax.random.normal(base_key, shape, dtype=jnp.float32)
    return jnp.clip(values, -256.0, 256.0).astype(jnp.bfloat16)


def draw_lengths(key, part):
    fill_key, pick_key = jax.random.split(jax.random.fold_in(key, 29))
    drawn = jax.random.randint(fill_key, (SEQS,), 2, CACHE + 1)
    chosen = jax.random.randint(pick_key, (SEQS // SEQ_DEV, 1), 0, SEQ_DEV)
    full_row = (jnp.arange(SEQ_DEV, dtype=jnp.int32)[None, :] == chosen).reshape(SEQS)
    return jnp.where(full_row, CACHE, drawn).astype(jnp.int32)


def shard_levels(own_key, dims, cuts, smallest, high):
    loudness = 1.0
    for axis_at, shards_of in cuts:
        steps = jax.random.uniform(jax.random.fold_in(jax.random.fold_in(own_key, 6), axis_at), (shards_of,), jnp.float32, smallest / len(cuts), high / len(cuts))
        loudness = loudness * jnp.repeat(jnp.exp(steps), dims[axis_at] // shards_of).reshape((-1,) + (1,) * (len(dims) - 1 - axis_at))
    return loudness


def centred(key, extent, scale, limit, cuts=(), held_as=jnp.bfloat16):
    loudness = shard_levels(key, extent, cuts, -0.22, 0.18) if cuts else 1.0
    values = jax.random.normal(key, extent, jnp.float32) * scale * loudness
    return jnp.minimum(jnp.maximum(values, -limit), limit).astype(held_as)


def setup_inputs(seed: int = 0) -> dict:
    arg_keys = jax.random.split(jax.random.key(seed), 10)
    hidden_state = draw_hidden_state(jax.random.fold_in(arg_keys[9], 71), 0)
    attn_gain = jnp.clip(1.0 + 0.1 * jax.random.normal(arg_keys[1], (D,), jnp.float32), 0.5, 1.5).astype(jnp.bfloat16)
    ffn_gain = jnp.clip(1.0 + 0.1 * jax.random.normal(arg_keys[2], (D,), jnp.float32), 0.5, 1.5).astype(jnp.bfloat16)
    w_query = centred(arg_keys[3], (D, HEADS * HD), (D // 4) ** -0.5, 0.125, ((0, 8), (1, 16)))
    w_keyval = centred(arg_keys[4], (D, 2 * KVH * HD), D ** -0.5, 0.0625, ((0, 8), (1, 16)))
    w_output = centred(arg_keys[5], (HEADS * HD, D), (HEADS * HD) ** -0.5, 0.0625, ((0, 16), (1, 8)))
    cache_keys = draw_cache_keys(jax.random.fold_in(arg_keys[9], 71), 0)
    cache_values = centred(arg_keys[7], (SEQS, KVH, CACHE, HD), 1.0, 6.0, ((0, 128),))
    lengths = draw_lengths(jax.random.fold_in(arg_keys[9], 71), 0)
    return dict(hidden_state=hidden_state, attn_gain=attn_gain, ffn_gain=ffn_gain, w_query=w_query, w_keyval=w_keyval, w_output=w_output, cache_keys=cache_keys, cache_values=cache_values, lengths=lengths)


epsilon = 1e-05
rope_base = 500000.0

def rotate(heads_block, position):
    head_dim = heads_block.shape[-1]
    half_dim = head_dim // 2
    frequency = rope_base ** (-2.0 * jnp.arange(half_dim, dtype=jnp.float32) / head_dim)
    angles = position.astype(jnp.float32)[:, None] * frequency[None, :]
    cosine = jnp.cos(angles)[:, None, :]
    sine_part = jnp.sin(angles)[:, None, :]
    lower_half = heads_block[..., :half_dim]
    upper_half = heads_block[..., half_dim:]
    return jnp.concatenate([lower_half * cosine - upper_half * sine_part, upper_half * cosine + lower_half * sine_part], axis=-1)

def attend(queries, fresh, cache_keys, cache_values, lengths):
    seq_count, kv_heads, cache_len, head_dim = cache_keys.shape
    q_heads = queries.shape[1] // head_dim
    q_per_kv = q_heads // kv_heads
    kv_width = kv_heads * head_dim
    grouped = queries.astype(jnp.float32).reshape(seq_count, kv_heads, q_per_kv, head_dim)
    new_keys = fresh[:, :kv_width].astype(jnp.float32).reshape(seq_count, kv_heads, head_dim)
    new_values = fresh[:, kv_width:].astype(jnp.float32).reshape(seq_count, kv_heads, head_dim)
    score_scale = head_dim ** (-0.5)
    scores = jnp.einsum('nkgd,nkld->nkgl', grouped, cache_keys.astype(jnp.float32)) * score_scale
    self_score = jnp.einsum('nkgd,nkd->nkg', grouped, new_keys) * score_scale
    live_mask = jnp.arange(cache_len, dtype=jnp.int32)[None, :] < lengths[:, None]
    scores = jnp.where(live_mask[:, None, None, :], scores, -1e+30)
    row_top = jnp.maximum(lax.optimization_barrier(jnp.max(scores, axis=3)), self_score)
    exp_scores = jnp.exp(scores - row_top[..., None])
    self_weight = jnp.exp(self_score - row_top)
    denom_sum = lax.optimization_barrier(jnp.sum(exp_scores, axis=3)) + self_weight
    weight_bf = (exp_scores / denom_sum[..., None]).astype(jnp.bfloat16)
    self_bf = (self_weight / denom_sum).astype(jnp.bfloat16)
    context = jnp.einsum('nkgl,nkld->nkgd', weight_bf.astype(jnp.float32), cache_values.astype(jnp.float32))
    context = context + self_bf.astype(jnp.float32)[..., None] * new_values[:, :, None, :]
    return context.reshape(seq_count, q_heads * head_dim).astype(jnp.bfloat16)

def reference(hidden_state, attn_gain, ffn_gain, w_query, w_keyval, w_output, cache_keys, cache_values, lengths):
    resident = hidden_state.astype(jnp.float32)
    inverse = lax.rsqrt(lax.optimization_barrier(jnp.mean(resident * resident, axis=1, keepdims=True)) + epsilon)
    normed = (resident * inverse * attn_gain.astype(jnp.float32)).astype(jnp.bfloat16)
    queries = jnp.dot(normed, w_query, preferred_element_type=jnp.float32)
    keyval = jnp.dot(normed, w_keyval, preferred_element_type=jnp.float32)
    seq_total = queries.shape[0]
    kv_width = KVH * HD
    roped_q = rotate(queries.reshape(seq_total, HEADS, HD), lengths).reshape(seq_total, HEADS * HD).astype(jnp.bfloat16)
    new_keys = rotate(keyval[:, :kv_width].reshape(seq_total, KVH, HD), lengths).reshape(seq_total, kv_width).astype(jnp.bfloat16)
    new_values = keyval[:, kv_width:].astype(jnp.bfloat16)
    fresh = jnp.concatenate([new_keys, new_values], axis=1)
    block_count = seq_total // SEQ_DEV

    def one_block(pieces):
        return attend(pieces[0], pieces[1], pieces[2], pieces[3], pieces[4])
    contexts = lax.map(one_block, (roped_q.reshape(block_count, SEQ_DEV, HEADS * HD), fresh.reshape(block_count, SEQ_DEV, 2 * kv_width), cache_keys.reshape(block_count, SEQ_DEV, KVH, CACHE, HD), cache_values.reshape(block_count, SEQ_DEV, KVH, CACHE, HD), lengths.reshape(block_count, SEQ_DEV)))
    context = contexts.reshape(seq_total, HEADS * HD)
    summed = jnp.dot(context, w_output, preferred_element_type=jnp.float32)
    branch = summed.astype(jnp.bfloat16)
    stream = resident + summed
    inverse_two = lax.rsqrt(lax.optimization_barrier(jnp.mean(stream * stream, axis=1, keepdims=True)) + epsilon)
    ffn_input = (stream * inverse_two * ffn_gain.astype(jnp.float32)).astype(jnp.bfloat16)
    return (branch, ffn_input)
```

```python
import jax
import jax.numpy as jnp
from jax import lax
from jax.sharding import Mesh, PartitionSpec as P

EPS = 1e-05
ROPE_BASE = 500000.0
F32 = jnp.float32
BF16 = jnp.bfloat16


CUBE = ("zl", "yl", "c")
PAIR = ("yl", "c")
WIDE = ("yh", "zh", "x")


def rotate(v, position):
    half = v.shape[-1] // 2
    freq = ROPE_BASE ** (-2.0 * jnp.arange(half, dtype=F32) / v.shape[-1])
    angles = position.astype(F32)[:, None] * freq[None, :]
    cos = jnp.cos(angles)[:, None, :]
    sin = jnp.sin(angles)[:, None, :]
    low, high = v[..., :half], v[..., half:]
    return jnp.concatenate([low * cos - high * sin, high * cos + low * sin], axis=-1)


def attend(grouped, new_keys, new_values, cache_keys, cache_values, lengths):
    n, kv_heads, cache_len, head_dim = cache_keys.shape
    scale = head_dim ** (-0.5)
    scores = jnp.einsum("nkgd,nkld->nkgl", grouped, cache_keys, preferred_element_type=F32) * scale
    self_score = jnp.einsum("nkgd,nkd->nkg", grouped, new_keys, preferred_element_type=F32) * scale
    live = jnp.arange(cache_len, dtype=jnp.int32)[None, :] < lengths[:, None]
    scores = jnp.where(live[:, None, None, :], scores, -1e30)
    top = jnp.maximum(jnp.max(scores, axis=3), self_score)
    e = jnp.exp(scores - top[..., None])
    e_self = jnp.exp(self_score - top)
    denom = jnp.sum(e, axis=3) + e_self
    weights = (e / denom[..., None]).astype(BF16)
    w_self = (e_self / denom).astype(BF16)
    context = jnp.einsum("nkgl,nkld->nkgd", weights, cache_values, preferred_element_type=F32)
    context = context + w_self.astype(F32)[..., None] * new_values.astype(F32)[:, :, None, :]
    return context.astype(BF16)


def xor_pairs(k):
    return [(i, i ^ k) for i in range(4)]


SWAP = [(g * 4 + x, x * 4 + g) for g in range(4) for x in range(4)]


def sum_over_x(v):
    return sum((lax.ppermute(v, "x", xor_pairs(k)) for k in (1, 2, 3)), v)


def local(h, attn_gain, ffn_gain, w_query, w_keyval, w_output, cache_keys, cache_values, lengths):
    x_pos = lax.axis_index("x")
    shard = lax.axis_index(("x", "yl", "c"))
    seq_dev, kv_heads, _, head_dim = cache_keys.shape
    tokens, width = h.shape
    quarter = tokens // 4
    model = 16 * width
    wide = 4 * width

    w_qkv = lax.all_gather(jnp.concatenate([w_query, w_keyval], axis=1), CUBE, axis=0)
    w_out = lax.all_gather(w_output, CUBE, axis=0)
    rows = w_qkv.shape[1]
    cols = w_qkv.shape[2]
    q_cols = w_query.shape[1]

    sent = h.reshape(4, 4, seq_dev, width).transpose(1, 0, 2, 3).reshape(4, quarter, width)
    got = lax.all_to_all(sent, PAIR, 0, 0, tiled=True)
    resident = got.transpose(1, 0, 2).reshape(quarter, wide).astype(F32)
    squares = sum_over_x(jnp.sum(resident * resident, axis=1))
    inverse = lax.rsqrt(squares / model + EPS)[:, None]
    gain = lax.dynamic_slice_in_dim(attn_gain, x_pos * wide, wide).astype(F32)
    normed = (resident * inverse * gain).astype(BF16)
    normed = lax.ppermute(normed, WIDE, SWAP)
    slots = [normed] + [lax.ppermute(normed, "x", xor_pairs(k)) for k in (1, 2, 3)]

    def placed(j):
        out = slots[j]
        for k in (1, 2, 3):
            out = jnp.where(x_pos == k, slots[j ^ k], out)
        return out

    lhs = jnp.concatenate([placed(j) for j in range(4)], axis=0)
    parts = []
    for p in range(4):
        acc = sum(
            jnp.dot(lhs[:, z * rows : (z + 1) * rows], w_qkv[z * 4 + p], preferred_element_type=F32)
            for z in range(2)
        )
        parts.append(acc.astype(BF16))
    partial = jnp.concatenate(parts, axis=1).reshape(16, seq_dev, 4 * cols)
    arrived = lax.all_to_all(partial, WIDE, 0, 0, tiled=True)
    qkv = jnp.sum(arrived.reshape(4, 4, seq_dev, 4, cols).astype(F32), axis=0)
    queries = qkv[..., :q_cols].transpose(1, 0, 2, 3).reshape(seq_dev, 16 * q_cols // head_dim, head_dim)
    keyval = qkv[..., q_cols:].transpose(1, 0, 2, 3).reshape(seq_dev, 2 * kv_heads, head_dim)
    own_len = lax.dynamic_slice_in_dim(lengths, shard * seq_dev, seq_dev)
    roped_q = rotate(queries, own_len).astype(BF16)
    new_keys = rotate(keyval[:, :kv_heads], own_len).astype(BF16)
    new_values = keyval[:, kv_heads:].astype(BF16)
    per_kv = roped_q.shape[1] // kv_heads
    grouped = roped_q.reshape(seq_dev, kv_heads, per_kv, head_dim)
    context = attend(grouped, new_keys, new_values, cache_keys, cache_values, own_len)

    context = context.reshape(seq_dev, 4, wide).transpose(1, 0, 2)
    context = jnp.broadcast_to(context[None], (4, 4, seq_dev, wide)).reshape(16, seq_dev, wide)
    context = lax.all_to_all(context, WIDE, 0, 0, tiled=True).reshape(tokens, wide)
    outs = []
    for z in range(2):
        acc = sum(
            jnp.dot(context[:, p * width : (p + 1) * width], w_out[z * 4 + p], preferred_element_type=F32)
            for p in range(4)
        )
        outs.append(acc.astype(BF16))
    out = jnp.concatenate(outs, axis=1).reshape(4, quarter, wide)
    out = lax.all_to_all(out, "x", 0, 0, tiled=True)
    out = jnp.sum(out.astype(F32), axis=0).astype(BF16)
    branch = lax.ppermute(out, WIDE, SWAP)
    stream = resident + branch.astype(F32)
    squares_two = sum_over_x(jnp.sum(stream * stream, axis=1))
    inverse_two = lax.rsqrt(squares_two / model + EPS)[:, None]
    gain_two = lax.dynamic_slice_in_dim(ffn_gain, x_pos * wide, wide).astype(F32)
    ffn_input = (stream * inverse_two * gain_two).astype(BF16)
    both = jnp.stack([branch, ffn_input]).reshape(2, quarter, 4, width).transpose(2, 0, 1, 3)
    both = lax.all_to_all(both, PAIR, 0, 0, tiled=True)
    both = both.reshape(4, 2, 4, seq_dev, width).transpose(1, 2, 0, 3, 4).reshape(2, tokens, width)
    return both[0], both[1]


def solution(mesh):
    fine = Mesh(mesh.devices.reshape(2, 2, 2, 4, 2, 2), ("yh", "zh", "zl", "x", "yl", "c"))
    group = ("yh", "zh", "zl")
    shard = ("x", "yl", "c")
    placed = (
        P(group, shard),
        P(),
        P(),
        P(group, shard),
        P(group, shard),
        P(shard, group),
        P(group + shard, None, None, None),
        P(group + shard, None, None, None),
        P(group),
    )
    return jax.shard_map(
        local,
        mesh=fine,
        in_specs=placed,
        out_specs=(P(group, shard), P(group, shard)),
        check_vma=False,
    )
```

```python
import jax
import jax.numpy as jnp
from jax import lax
from jax.sharding import Mesh, PartitionSpec as P

EPS = 1e-05
ROPE_BASE = 500000.0
F32 = jnp.float32
BF16 = jnp.bfloat16


CUBE = ("zl", "yl", "c")
PAIR = ("yl", "c")
WIDE = ("yh", "zh", "x")


def rotate(v, position):
    half = v.shape[-1] // 2
    freq = ROPE_BASE ** (-2.0 * jnp.arange(half, dtype=F32) / v.shape[-1])
    angles = position.astype(F32)[:, None] * freq[None, :]
    cos = jnp.cos(angles)[:, None, :]
    sin = jnp.sin(angles)[:, None, :]
    low, high = v[..., :half], v[..., half:]
    return jnp.concatenate([low * cos - high * sin, high * cos + low * sin], axis=-1)


def attend(grouped, new_keys, new_values, cache_keys, cache_values, lengths):
    n, kv_heads, cache_len, head_dim = cache_keys.shape
    scale = head_dim ** (-0.5)
    scores = jnp.einsum("nkgd,nkld->nkgl", grouped, cache_keys, preferred_element_type=F32) * scale
    self_score = jnp.einsum("nkgd,nkd->nkg", grouped, new_keys, preferred_element_type=F32) * scale
    live = jnp.arange(cache_len, dtype=jnp.int32)[None, :] < lengths[:, None]
    scores = jnp.where(live[:, None, None, :], scores, -1e30)
    top = jnp.maximum(jnp.max(scores, axis=3), self_score)
    e = jnp.exp(scores - top[..., None])
    e_self = jnp.exp(self_score - top)
    denom = jnp.sum(e, axis=3) + e_self
    weights = (e / denom[..., None]).astype(BF16)
    w_self = (e_self / denom).astype(BF16)
    context = jnp.einsum("nkgl,nkld->nkgd", weights, cache_values, preferred_element_type=F32)
    context = context + w_self.astype(F32)[..., None] * new_values.astype(F32)[:, :, None, :]
    return context.astype(BF16)


def xor_pairs(k):
    return [(i, i ^ k) for i in range(4)]


SPREAD = [(g * 4 + x, x * 4 + (g ^ x)) for g in range(4) for x in range(4)]
COLLECT = [(g * 4 + x, (x ^ 1) * 4 + g) for g in range(4) for x in range(4)]
FLIP = [(0, 1), (1, 0)]


def swap(v, axis):
    return lax.ppermute(v, axis, FLIP)


def cube_of(w):
    half = w.shape[0] // 2
    far_z, far_y = swap(w, "zl"), swap(w, "yl")
    both = jnp.concatenate([swap(far_z[:half], "yl"), swap(far_y[half:], "zl")], axis=0)
    return [[[v, swap(v, "c")] for v in pair] for pair in ((w, far_y), (far_z, both))]


def unrelated(pieces, index):
    n = len(pieces)
    out = []
    for j in range(n):
        v = pieces[j]
        for k in range(1, n):
            v = jnp.where(index == k, pieces[j ^ k], v)
        out.append(v)
    return out


def sum_over_x(v):
    return sum((lax.ppermute(v, "x", xor_pairs(k)) for k in (1, 2, 3)), v)


def local(h, attn_gain, ffn_gain, w_query, w_keyval, w_output, cache_keys, cache_values, lengths):
    x_pos = lax.axis_index("x")
    shard = lax.axis_index(("x", "yl", "c"))
    seq_dev, kv_heads, _, head_dim = cache_keys.shape
    tokens, width = h.shape
    quarter = tokens // 4
    model = 16 * width
    wide = 4 * width

    q_cols = w_query.shape[1]
    rows, cols = w_query.shape[0], q_cols + w_keyval.shape[1]
    w_qkv = cube_of(jnp.concatenate([w_query, w_keyval], axis=1))
    w_out = cube_of(w_output)

    sent = h.reshape(4, 4, seq_dev, width).transpose(1, 0, 2, 3).reshape(4, quarter, width)
    got = lax.all_to_all(sent, PAIR, 0, 0, tiled=True)
    resident = got.transpose(1, 0, 2).reshape(quarter, wide).astype(F32)
    squares = sum_over_x(jnp.sum(resident * resident, axis=1))
    inverse = lax.rsqrt(squares / model + EPS)[:, None]
    gain = lax.dynamic_slice_in_dim(attn_gain, x_pos * wide, wide).astype(F32)
    normed = (resident * inverse * gain).astype(BF16)
    z_pos = lax.axis_index("zl")
    normed = jnp.concatenate(unrelated([normed[:, :rows], normed[:, rows:]], z_pos), axis=1)
    normed = lax.ppermute(normed, WIDE, SPREAD)
    slots = [normed] + [lax.ppermute(normed, "x", xor_pairs(k)) for k in (1, 2, 3)]

    order = lax.axis_index("x") ^ lax.axis_index(("yh", "zh"))
    lhs = lax.optimization_barrier(jnp.concatenate(unrelated(slots, order), axis=0))
    parts = []
    for dy in range(2):
        for dc in range(2):
            acc = sum(
                jnp.dot(lhs[:, z * rows : (z + 1) * rows], w_qkv[z][dy][dc], preferred_element_type=F32)
                for z in range(2)
            )
            parts.append(acc.astype(BF16))
    partial = jnp.concatenate(parts, axis=1).reshape(16, seq_dev, 4 * cols)
    arrived = lax.all_to_all(partial, WIDE, 0, 0, tiled=True)
    qkv = jnp.sum(arrived.reshape(4, 4, seq_dev, 4 * cols).astype(F32), axis=0)
    pair_pos = lax.axis_index(PAIR)
    q_of = [unrelated([qkv[x, :, p * cols : p * cols + q_cols] for p in range(4)], pair_pos) for x in range(4)]
    kv_of = [unrelated([qkv[x, :, p * cols + q_cols : (p + 1) * cols] for p in range(4)], pair_pos) for x in range(4)]
    queries = jnp.concatenate([v for x in q_of for v in x], axis=1).reshape(seq_dev, -1, head_dim)
    keyval = jnp.concatenate([v for x in kv_of for v in x], axis=1).reshape(seq_dev, -1, head_dim)
    own_len = lax.dynamic_slice_in_dim(lengths, shard * seq_dev, seq_dev)
    roped_q = rotate(queries, own_len).astype(BF16)
    new_keys = rotate(keyval[:, :kv_heads], own_len).astype(BF16)
    new_values = keyval[:, kv_heads:].astype(BF16)
    per_kv = roped_q.shape[1] // kv_heads
    grouped = roped_q.reshape(seq_dev, kv_heads, per_kv, head_dim)
    context = attend(grouped, new_keys, new_values, cache_keys, cache_values, own_len)

    context = context.reshape(seq_dev, 4, wide).transpose(1, 0, 2)
    context = jnp.broadcast_to(context[None], (4, 4, seq_dev, wide)).reshape(16, seq_dev, wide)
    context = lax.all_to_all(context, WIDE, 0, 0, tiled=True).reshape(tokens, wide)
    blocks = unrelated([context[:, p * width : (p + 1) * width] for p in range(4)], pair_pos)
    outs = []
    for z in range(2):
        acc = sum(
            jnp.dot(blocks[p], w_out[z][p // 2][p % 2], preferred_element_type=F32) for p in range(4)
        )
        outs.append(acc.astype(BF16))
    outs = unrelated(outs, z_pos)
    out = jnp.concatenate(outs, axis=1).reshape(4, quarter, wide)
    out = jnp.stack([out[j ^ 1] for j in range(4)])
    out = lax.all_to_all(out, "x", 0, 0, tiled=True)
    out = jnp.sum(out.astype(F32), axis=0).astype(BF16)
    branch = lax.ppermute(out, WIDE, COLLECT)
    stream = resident + branch.astype(F32)
    squares_two = sum_over_x(jnp.sum(stream * stream, axis=1))
    inverse_two = lax.rsqrt(squares_two / model + EPS)[:, None]
    gain_two = lax.dynamic_slice_in_dim(ffn_gain, x_pos * wide, wide).astype(F32)
    ffn_input = (stream * inverse_two * gain_two).astype(BF16)
    both = jnp.stack([branch, ffn_input]).reshape(2, quarter, 4, width).transpose(2, 0, 1, 3)
    both = lax.all_to_all(both, PAIR, 0, 0, tiled=True)
    both = both.reshape(4, 2, 4, seq_dev, width).transpose(1, 2, 0, 3, 4).reshape(2, tokens, width)
    return both[0], both[1]


def solution(mesh):
    fine = Mesh(mesh.devices.reshape(2, 2, 2, 4, 2, 2), ("yh", "zh", "zl", "x", "yl", "c"))
    group = ("yh", "zh", "zl")
    shard = ("x", "yl", "c")
    placed = (
        P(group, shard),
        P(),
        P(),
        P(group, shard),
        P(group, shard),
        P(shard, group),
        P(group + shard, None, None, None),
        P(group + shard, None, None, None),
        P(group),
    )
    return jax.shard_map(
        local,
        mesh=fine,
        in_specs=placed,
        out_specs=(P(group, shard), P(group, shard)),
        check_vma=False,
    )
```

```python
import jax
import jax.numpy as jnp
from jax import lax
from jax.experimental import pallas as pl
from jax.experimental.pallas import tpu as pltpu
from jax.sharding import Mesh, PartitionSpec as P

EPS = 1e-05
ROPE_BASE = 500000.0
F32 = jnp.float32
BF16 = jnp.bfloat16


PAIR = ("yl", "c")
WIDE = ("yh", "zh", "x")


def rotate(v, position):
    half = v.shape[-1] // 2
    freq = ROPE_BASE ** (-2.0 * jnp.arange(half, dtype=F32) / v.shape[-1])
    angles = position.astype(F32)[:, None] * freq[None, :]
    cos = jnp.cos(angles)[:, None, :]
    sin = jnp.sin(angles)[:, None, :]
    low, high = v[..., :half], v[..., half:]
    return jnp.concatenate([low * cos - high * sin, high * cos + low * sin], axis=-1)


def attend(grouped, new_keys, new_values, cache_keys, cache_values, lengths):
    _, _, cache_len, head_dim = cache_keys.shape
    scale = head_dim ** (-0.5)
    scores = jnp.einsum("nkgd,nkld->nkgl", grouped, cache_keys, preferred_element_type=F32) * scale
    self_score = jnp.einsum("nkgd,nkd->nkg", grouped, new_keys, preferred_element_type=F32) * scale
    live = jnp.arange(cache_len, dtype=jnp.int32)[None, :] < lengths[:, None]
    scores = jnp.where(live[:, None, None, :], scores, -1e30)
    top = jnp.maximum(jnp.max(scores, axis=3), self_score)
    e = jnp.exp(scores - top[..., None])
    e_self = jnp.exp(self_score - top)
    denom = jnp.sum(e, axis=3) + e_self
    weights = (e / denom[..., None]).astype(BF16)
    w_self = (e_self / denom).astype(BF16)
    context = jnp.einsum("nkgl,nkld->nkgd", weights, cache_values, preferred_element_type=F32)
    context = context + w_self.astype(F32)[..., None] * new_values.astype(F32)[:, :, None, :]
    return context.astype(BF16)


def xor_pairs(k):
    return [(i, i ^ k) for i in range(4)]


SPREAD = [(g * 4 + x, x * 4 + (g ^ x)) for g in range(4) for x in range(4)]
COLLECT = [(g * 4 + x, (x ^ 1) * 4 + g) for g in range(4) for x in range(4)]
FLIP = [(0, 1), (1, 0)]


def swap(v, axis):
    return lax.ppermute(v, axis, FLIP)


def cube_of(w):
    half = w.shape[0] // 2
    far_z, far_y = swap(w, "zl"), swap(w, "yl")
    top, bottom = swap(far_z[:half], "yl"), swap(far_y[half:], "zl")
    pieces = []
    for dz, dy, row, v in ((0, 0, 0, w), (1, 0, 0, far_z), (0, 1, 0, far_y), (1, 1, 0, top), (1, 1, half, bottom)):
        pieces += [(dz, dy, 0, row, v), (dz, dy, 1, row, swap(v, "c"))]
    return pieces


def matmul_kernel(lhs_pieces, weights, out_shape, place, finish, scalars):
    n = len(weights)

    def body(scalar_ref, *refs):
        lhs_refs, w_refs = refs[: len(lhs_pieces)], refs[len(lhs_pieces) : len(lhs_pieces) + n]
        out_ref, lhs_scr = refs[len(lhs_pieces) + n], refs[len(lhs_pieces) + n + 1]
        bufs, sem = refs[len(lhs_pieces) + n + 2 : -1], refs[-1]
        copies = [pltpu.make_async_copy(w_refs[i], bufs[i], sem.at[i]) for i in range(n)]
        for copy in copies:
            copy.start()
        place(scalar_ref, lhs_refs, lhs_scr)
        slots = sorted({slot for _, slot, _ in weights})
        for slot in slots:
            acc = None
            for i, (col, at, w) in enumerate(weights):
                if at != slot:
                    continue
                copies[i].wait()
                term = jnp.dot(lhs_scr[:, col : col + w.shape[0]], bufs[i][...], preferred_element_type=F32)
                acc = term if acc is None else acc + term
            finish(scalar_ref, out_ref, slot, acc.astype(BF16))

    rows = sum(v.shape[0] for v in lhs_pieces)
    depth = lhs_pieces[0].shape[1]
    flops = sum(2 * rows * w.size for _, _, w in weights)
    return pl.pallas_call(
        body,
        out_shape=jax.ShapeDtypeStruct(out_shape, BF16),
        in_specs=[pl.BlockSpec(memory_space=pltpu.SMEM)]
        + [pl.BlockSpec(memory_space=pltpu.VMEM)] * len(lhs_pieces)
        + [pl.BlockSpec(memory_space=pltpu.HBM)] * n,
        out_specs=pl.BlockSpec(memory_space=pltpu.VMEM),
        scratch_shapes=[pltpu.VMEM((rows, depth), BF16)]
        + [pltpu.VMEM(w.shape, BF16) for _, _, w in weights]
        + [pltpu.SemaphoreType.DMA((n,))],
        compiler_params=pltpu.CompilerParams(vmem_limit_bytes=30 << 20),
        cost_estimate=pl.CostEstimate(flops=flops, bytes_accessed=sum(2 * w.size for _, _, w in weights), transcendentals=0),
    )(jnp.stack(scalars).astype(jnp.int32), *lhs_pieces, *[w for _, _, w in weights])


def unrelated(pieces, index):
    n = len(pieces)
    out = []
    for j in range(n):
        v = pieces[j]
        for k in range(1, n):
            v = jnp.where(index == k, pieces[j ^ k], v)
        out.append(v)
    return out


def sum_over_x(v):
    return sum((lax.ppermute(v, "x", xor_pairs(k)) for k in (1, 2, 3)), v)


def local(h, attn_gain, ffn_gain, w_query, w_keyval, w_output, cache_keys, cache_values, lengths):
    x_pos = lax.axis_index("x")
    shard = lax.axis_index(("x", "yl", "c"))
    seq_dev, kv_heads, _, head_dim = cache_keys.shape
    tokens, width = h.shape
    quarter = tokens // 4
    model = 16 * width
    wide = 4 * width

    q_cols = w_query.shape[1]
    rows, cols = w_query.shape[0], q_cols + w_keyval.shape[1]
    w_qkv = cube_of(jnp.concatenate([w_query, w_keyval], axis=1))
    w_out = cube_of(w_output)

    sent = h.reshape(4, 4, seq_dev, width).transpose(1, 0, 2, 3).reshape(4, quarter, width)
    got = lax.all_to_all(sent, PAIR, 0, 0, tiled=True)
    resident = got.transpose(1, 0, 2).reshape(quarter, wide).astype(F32)
    squares = sum_over_x(jnp.sum(resident * resident, axis=1))
    inverse = lax.rsqrt(squares / model + EPS)[:, None]
    gain = lax.dynamic_slice_in_dim(attn_gain, x_pos * wide, wide).astype(F32)
    normed = (resident * inverse * gain).astype(BF16)
    z_pos = lax.axis_index("zl")
    normed = jnp.concatenate(unrelated([normed[:, :rows], normed[:, rows:]], z_pos), axis=1)
    normed = lax.ppermute(normed, WIDE, SPREAD)
    slots = [normed] + [lax.ppermute(normed, "x", xor_pairs(k)) for k in (1, 2, 3)]

    order = lax.axis_index("x") ^ lax.axis_index(("yh", "zh"))

    def place_tokens(scalar_ref, lhs_refs, lhs_scr):
        for k, ref in enumerate(lhs_refs):
            at = pl.multiple_of((scalar_ref[0] ^ k) * quarter, quarter)
            lhs_scr[pl.ds(at, quarter), :] = ref[...]

    def put_columns(scalar_ref, out_ref, slot, value):
        out_ref[:, slot * cols : (slot + 1) * cols] = value

    partial = matmul_kernel(
        slots,
        [(dz * rows + row, dy * 2 + dc, v) for dz, dy, dc, row, v in w_qkv],
        (tokens, 4 * cols),
        place_tokens,
        put_columns,
        [order],
    ).reshape(16, seq_dev, 4 * cols)
    arrived = lax.all_to_all(partial, WIDE, 0, 0, tiled=True)
    qkv = jnp.sum(arrived.reshape(4, 4, seq_dev, 4 * cols).astype(F32), axis=0)
    pair_pos = lax.axis_index(PAIR)
    q_of = [unrelated([qkv[x, :, p * cols : p * cols + q_cols] for p in range(4)], pair_pos) for x in range(4)]
    kv_of = [unrelated([qkv[x, :, p * cols + q_cols : (p + 1) * cols] for p in range(4)], pair_pos) for x in range(4)]
    queries = jnp.concatenate([v for x in q_of for v in x], axis=1).reshape(seq_dev, -1, head_dim)
    keyval = jnp.concatenate([v for x in kv_of for v in x], axis=1).reshape(seq_dev, -1, head_dim)
    own_len = lax.dynamic_slice_in_dim(lengths, shard * seq_dev, seq_dev)
    roped_q = rotate(queries, own_len).astype(BF16)
    new_keys = rotate(keyval[:, :kv_heads], own_len).astype(BF16)
    new_values = keyval[:, kv_heads:].astype(BF16)
    per_kv = roped_q.shape[1] // kv_heads
    grouped = roped_q.reshape(seq_dev, kv_heads, per_kv, head_dim)
    context = attend(grouped, new_keys, new_values, cache_keys, cache_values, own_len)

    context = context.reshape(seq_dev, 4, wide).transpose(1, 0, 2)
    context = jnp.broadcast_to(context[None], (4, 4, seq_dev, wide)).reshape(16, seq_dev, wide)
    context = lax.all_to_all(context, WIDE, 0, 0, tiled=True).reshape(tokens, wide)

    def place_heads(scalar_ref, lhs_refs, lhs_scr):
        for p in range(4):
            at = pl.multiple_of((scalar_ref[0] ^ p) * width, width)
            lhs_scr[:, p * width : (p + 1) * width] = lhs_refs[0][:, pl.ds(at, width)]

    def put_blocks(scalar_ref, out_ref, slot, value):
        n = value.shape[1]
        at = pl.multiple_of((scalar_ref[1] ^ slot) * n, n)
        for j in range(4):
            out_ref[j ^ 1, :, pl.ds(at, n)] = value[j * quarter : (j + 1) * quarter]

    out = matmul_kernel(
        [context],
        [((dy * 2 + dc) * width + row, dz, v) for dz, dy, dc, row, v in w_out],
        (4, quarter, wide),
        place_heads,
        put_blocks,
        [pair_pos, z_pos],
    )
    out = lax.all_to_all(out, "x", 0, 0, tiled=True)
    out = jnp.sum(out.astype(F32), axis=0).astype(BF16)
    branch = lax.ppermute(out, WIDE, COLLECT)
    stream = resident + branch.astype(F32)
    squares_two = sum_over_x(jnp.sum(stream * stream, axis=1))
    inverse_two = lax.rsqrt(squares_two / model + EPS)[:, None]
    gain_two = lax.dynamic_slice_in_dim(ffn_gain, x_pos * wide, wide).astype(F32)
    ffn_input = (stream * inverse_two * gain_two).astype(BF16)
    both = jnp.stack([branch, ffn_input]).reshape(2, quarter, 4, width).transpose(2, 0, 1, 3)
    both = lax.all_to_all(both, PAIR, 0, 0, tiled=True)
    both = both.reshape(4, 2, 4, seq_dev, width).transpose(1, 2, 0, 3, 4).reshape(2, tokens, width)
    return both[0], both[1]


def solution(mesh):
    fine = Mesh(mesh.devices.reshape(2, 2, 2, 4, 2, 2), ("yh", "zh", "zl", "x", "yl", "c"))
    group = ("yh", "zh", "zl")
    shard = ("x", "yl", "c")
    placed = (
        P(group, shard),
        P(),
        P(),
        P(group, shard),
        P(group, shard),
        P(shard, group),
        P(group + shard, None, None, None),
        P(group + shard, None, None, None),
        P(group),
    )
    return jax.shard_map(
        local,
        mesh=fine,
        in_specs=placed,
        out_specs=(P(group, shard), P(group, shard)),
        check_vma=False,
    )
```

```python
import jax
import jax.numpy as jnp
from jax import lax
from jax.experimental import pallas as pl
from jax.experimental.pallas import tpu as pltpu
from jax.sharding import Mesh, PartitionSpec as P

EPS = 1e-05
ROPE_BASE = 500000.0
F32 = jnp.float32
BF16 = jnp.bfloat16


PAIR = ("yl", "c")
WIDE = ("yh", "zh", "x")


def rotate(v, position):
    half = v.shape[-1] // 2
    freq = ROPE_BASE ** (-2.0 * jnp.arange(half, dtype=F32) / v.shape[-1])
    angles = position.astype(F32)[:, None] * freq[None, :]
    cos = jnp.cos(angles)[:, None, :]
    sin = jnp.sin(angles)[:, None, :]
    low, high = v[..., :half], v[..., half:]
    return jnp.concatenate([low * cos - high * sin, high * cos + low * sin], axis=-1)


def attend(grouped, new_keys, new_values, cache_keys, cache_values, lengths):
    _, _, cache_len, head_dim = cache_keys.shape
    scale = head_dim ** (-0.5)
    scores = jnp.einsum("nkgd,nkld->nkgl", grouped, cache_keys, preferred_element_type=F32) * scale
    self_score = jnp.einsum("nkgd,nkd->nkg", grouped, new_keys, preferred_element_type=F32) * scale
    live = jnp.arange(cache_len, dtype=jnp.int32)[None, :] < lengths[:, None]
    scores = jnp.where(live[:, None, None, :], scores, -1e30)
    top = jnp.maximum(jnp.max(scores, axis=3), self_score)
    e = jnp.exp(scores - top[..., None])
    e_self = jnp.exp(self_score - top)
    denom = jnp.sum(e, axis=3) + e_self
    weights = (e / denom[..., None]).astype(BF16)
    w_self = (e_self / denom).astype(BF16)
    context = jnp.einsum("nkgl,nkld->nkgd", weights, cache_values, preferred_element_type=F32)
    context = context + w_self.astype(F32)[..., None] * new_values.astype(F32)[:, :, None, :]
    return context.astype(BF16)


def xor_pairs(k):
    return [(i, i ^ k) for i in range(4)]


SPREAD = [(g * 4 + x, x * 4 + (g ^ x)) for g in range(4) for x in range(4)]
FLIP = [(0, 1), (1, 0)]
CHIP = ("x", "yl")
BLOCK = ("yh", "zh", "zl")
ACROSS = ("yh", "zh", "zl", "yl")


def swap(v, axis):
    return lax.ppermute(v, axis, FLIP)


def cube_of(w):
    half = w.shape[0] // 2
    far_z, far_y = swap(w, "zl"), swap(w, "yl")
    top, bottom = swap(far_z[:half], "yl"), swap(far_y[half:], "zl")
    pieces = []
    for dz, dy, row, v in ((0, 0, 0, w), (1, 0, 0, far_z), (0, 1, 0, far_y), (1, 1, 0, top), (1, 1, half, bottom)):
        pieces += [(dz, dy, 0, row, v), (dz, dy, 1, row, swap(v, "c"))]
    return pieces


def row_of(w):
    near = {k: lax.ppermute(w, "x", xor_pairs(k)) for k in (1, 3)}
    near[2] = lax.ppermute(w, "x", xor_pairs(2))
    near[0] = w
    pieces = []
    for k in (0, 1, 3, 2):
        pieces += [(k, 0, near[k]), (k, 1, swap(near[k], "c"))]
    return pieces


def matmul_kernel(lhs_pieces, weights, out_shape, place, finish, scalars):
    n = len(weights)

    def body(scalar_ref, *refs):
        lhs_refs, w_refs = refs[: len(lhs_pieces)], refs[len(lhs_pieces) : len(lhs_pieces) + n]
        out_ref, lhs_scr = refs[len(lhs_pieces) + n], refs[len(lhs_pieces) + n + 1]
        bufs, sem = refs[len(lhs_pieces) + n + 2 : -1], refs[-1]
        copies = [pltpu.make_async_copy(w_refs[i], bufs[i], sem.at[i]) for i in range(n)]
        for copy in copies:
            copy.start()
        if place is None:
            lhs_scr = lhs_refs[0]
        else:
            place(scalar_ref, lhs_refs, lhs_scr)
        slots = sorted({slot for _, slot, _ in weights})
        for slot in slots:
            acc = None
            for i, (col, home, w) in enumerate(weights):
                if home != slot:
                    continue
                copies[i].wait()
                if callable(col):
                    at = pl.ds(pl.multiple_of(col(scalar_ref), 128), w.shape[0])
                else:
                    at = slice(col, col + w.shape[0])
                term = jnp.dot(lhs_scr[:, at], bufs[i][...], preferred_element_type=F32)
                acc = term if acc is None else acc + term
            finish(scalar_ref, out_ref, slot, acc.astype(BF16))

    rows = sum(v.shape[0] for v in lhs_pieces)
    depth = lhs_pieces[0].shape[1]
    flops = sum(2 * rows * w.size for _, _, w in weights)
    return pl.pallas_call(
        body,
        out_shape=jax.ShapeDtypeStruct(out_shape, BF16),
        in_specs=[pl.BlockSpec(memory_space=pltpu.SMEM)]
        + [pl.BlockSpec(memory_space=pltpu.VMEM)] * len(lhs_pieces)
        + [pl.BlockSpec(memory_space=pltpu.HBM)] * n,
        out_specs=pl.BlockSpec(memory_space=pltpu.VMEM),
        scratch_shapes=[pltpu.VMEM((rows, depth) if place else (8, 128), BF16)]
        + [pltpu.VMEM(w.shape, BF16) for _, _, w in weights]
        + [pltpu.SemaphoreType.DMA((n,))],
        compiler_params=pltpu.CompilerParams(vmem_limit_bytes=30 << 20),
        cost_estimate=pl.CostEstimate(flops=flops, bytes_accessed=sum(2 * w.size for _, _, w in weights), transcendentals=0),
    )(jnp.stack(scalars).astype(jnp.int32), *lhs_pieces, *[w for _, _, w in weights])


def unrelated(pieces, index):
    n = len(pieces)
    out = []
    for j in range(n):
        v = pieces[j]
        for k in range(1, n):
            v = jnp.where(index == k, pieces[j ^ k], v)
        out.append(v)
    return out


def sum_over_x(v):
    return sum((lax.ppermute(v, "x", xor_pairs(k)) for k in (1, 2, 3)), v)


def local(h, attn_gain, ffn_gain, w_query, w_keyval, w_output, cache_keys, cache_values, lengths):
    x_pos = lax.axis_index("x")
    shard = lax.axis_index(("x", "yl", "c"))
    seq_dev, kv_heads, _, head_dim = cache_keys.shape
    tokens, width = h.shape
    quarter = tokens // 4
    model = 16 * width
    wide = 4 * width

    q_cols = w_query.shape[1]
    rows, cols = w_query.shape[0], q_cols + w_keyval.shape[1]
    w_qkv = cube_of(jnp.concatenate([w_query, w_keyval], axis=1))
    w_out = row_of(w_output)

    sent = h.reshape(4, 4, seq_dev, width).transpose(1, 0, 2, 3).reshape(4, quarter, width)
    got = lax.all_to_all(sent, PAIR, 0, 0, tiled=True)
    core = lax.axis_index("c")
    by_core = h.reshape(8, 2, seq_dev, width)
    mine = lax.dynamic_index_in_dim(by_core, core, 1, keepdims=False).reshape(-1, width)
    other = swap(lax.dynamic_index_in_dim(by_core, 1 - core, 1, keepdims=False), "c").reshape(-1, width)
    home_rows = jnp.concatenate(unrelated([mine, other], core), axis=1)
    resident = got.transpose(1, 0, 2).reshape(quarter, wide).astype(F32)
    squares = sum_over_x(jnp.sum(resident * resident, axis=1))
    inverse = lax.rsqrt(squares / model + EPS)[:, None]
    gain = lax.dynamic_slice_in_dim(attn_gain, x_pos * wide, wide).astype(F32)
    normed = (resident * inverse * gain).astype(BF16)
    z_pos = lax.axis_index("zl")
    normed = jnp.concatenate(unrelated([normed[:, :rows], normed[:, rows:]], z_pos), axis=1)
    normed = lax.ppermute(normed, WIDE, SPREAD)
    slots = [normed] + [lax.ppermute(normed, "x", xor_pairs(k)) for k in (1, 2, 3)]

    order = lax.axis_index("x") ^ lax.axis_index(("yh", "zh"))

    def place_tokens(scalar_ref, lhs_refs, lhs_scr):
        for k, ref in enumerate(lhs_refs):
            at = pl.multiple_of((scalar_ref[0] ^ k) * quarter, quarter)
            lhs_scr[pl.ds(at, quarter), :] = ref[...]

    def put_columns(scalar_ref, out_ref, slot, value):
        out_ref[:, slot * cols : (slot + 1) * cols] = value

    partial = matmul_kernel(
        slots,
        [(dz * rows + row, dy * 2 + dc, v) for dz, dy, dc, row, v in w_qkv],
        (tokens, 4 * cols),
        place_tokens,
        put_columns,
        [order],
    ).reshape(16, seq_dev, 4 * cols)
    arrived = lax.all_to_all(partial, WIDE, 0, 0, tiled=True)
    qkv = jnp.sum(arrived.reshape(4, 4, seq_dev, 4 * cols).astype(F32), axis=0)
    pair_pos = lax.axis_index(PAIR)
    q_of = [unrelated([qkv[x, :, p * cols : p * cols + q_cols] for p in range(4)], pair_pos) for x in range(4)]
    kv_of = [unrelated([qkv[x, :, p * cols + q_cols : (p + 1) * cols] for p in range(4)], pair_pos) for x in range(4)]
    queries = jnp.concatenate([v for x in q_of for v in x], axis=1).reshape(seq_dev, -1, head_dim)
    keyval = jnp.concatenate([v for x in kv_of for v in x], axis=1).reshape(seq_dev, -1, head_dim)
    own_len = lax.dynamic_slice_in_dim(lengths, shard * seq_dev, seq_dev)
    roped_q = rotate(queries, own_len).astype(BF16)
    new_keys = rotate(keyval[:, :kv_heads], own_len).astype(BF16)
    new_values = keyval[:, kv_heads:].astype(BF16)
    per_kv = roped_q.shape[1] // kv_heads
    grouped = roped_q.reshape(seq_dev, kv_heads, per_kv, head_dim)
    context = attend(grouped, new_keys, new_values, cache_keys, cache_values, own_len)

    context = context.reshape(seq_dev, 4, 2, 2 * width).transpose(2, 0, 1, 3).reshape(1, 2, seq_dev, 2 * wide)
    context = jnp.broadcast_to(context, (8, 2, seq_dev, 2 * wide)).reshape(16, seq_dev, 2 * wide)
    context = lax.all_to_all(context, ACROSS, 0, 0, tiled=True).reshape(tokens, 2 * wide)
    out_cols = w_output.shape[1]
    chip = lax.axis_index(CHIP)
    part = 2 * seq_dev

    def column_of(dx, dc):
        return lambda scalar_ref: ((scalar_ref[0] ^ dx) * 2 + (scalar_ref[1] ^ dc)) * width

    def put_blocks(scalar_ref, out_ref, slot, value):
        for g in range(8):
            out_ref[g] = value[g * part : (g + 1) * part]

    out = matmul_kernel(
        [context],
        [(column_of(dx, dc), 0, v) for dx, dc, v in w_out],
        (8, part, out_cols),
        None,
        put_blocks,
        [x_pos, core],
    )
    out = lax.all_to_all(out, BLOCK, 0, 0, tiled=True)
    out = lax.all_to_all(out, CHIP, 0, 0, tiled=True)
    summed = jnp.sum(out.reshape(4, 2, part, out_cols).astype(F32), axis=1).reshape(tokens // 2, out_cols)
    stream = home_rows.astype(F32) + summed
    squares_two = jnp.sum(stream * stream, axis=1)
    squares_two = lax.all_to_all(jnp.broadcast_to(squares_two[None], (8, tokens // 2)), CHIP, 0, 0, tiled=True)
    inverse_two = lax.rsqrt(jnp.sum(squares_two, axis=0) / model + EPS)[:, None]
    gain_two = lax.dynamic_slice_in_dim(ffn_gain, chip * out_cols, out_cols).astype(F32)
    ffn_input = (stream * inverse_two * gain_two).astype(BF16)
    both = jnp.stack([summed.astype(BF16), ffn_input]).reshape(2, tokens // 2, 2, width)
    keep = lax.dynamic_index_in_dim(both, core, 2, keepdims=False)
    came = swap(lax.dynamic_index_in_dim(both, 1 - core, 2, keepdims=False), "c")
    both = unrelated([v.reshape(2, 8, seq_dev, width) for v in (keep, came)], core)
    both = jnp.stack(both, axis=2).reshape(2, tokens, width)
    return both[0], both[1]


def solution(mesh):
    fine = Mesh(mesh.devices.reshape(2, 2, 2, 4, 2, 2), ("yh", "zh", "zl", "x", "yl", "c"))
    group = ("yh", "zh", "zl")
    shard = ("x", "yl", "c")
    placed = (
        P(group, shard),
        P(),
        P(),
        P(group, shard),
        P(group, shard),
        P(shard, group),
        P(group + shard, None, None, None),
        P(group + shard, None, None, None),
        P(group),
    )
    return jax.shard_map(
        local,
        mesh=fine,
        in_specs=placed,
        out_specs=(P(group, shard), P(group, shard)),
        check_vma=False,
    )
```

```python
import jax
import jax.numpy as jnp
from jax import lax
from jax.experimental import pallas as pl
from jax.experimental.pallas import tpu as pltpu
from jax.sharding import Mesh, PartitionSpec as P

EPS = 1e-05
ROPE_BASE = 500000.0
F32 = jnp.float32
BF16 = jnp.bfloat16


PAIR = ("yl", "c")
WIDE = ("yh", "zh", "x")


def rotate(v, position):
    half = v.shape[-1] // 2
    freq = ROPE_BASE ** (-2.0 * jnp.arange(half, dtype=F32) / v.shape[-1])
    angles = position.astype(F32)[:, None] * freq[None, :]
    cos = jnp.cos(angles)[:, None, :]
    sin = jnp.sin(angles)[:, None, :]
    low, high = v[..., :half], v[..., half:]
    return jnp.concatenate([low * cos - high * sin, high * cos + low * sin], axis=-1)


def attend(grouped, new_keys, new_values, cache_keys, cache_values, lengths):
    _, _, cache_len, head_dim = cache_keys.shape
    scale = head_dim ** (-0.5)
    scores = jnp.einsum("nkgd,nkld->nkgl", grouped, cache_keys, preferred_element_type=F32) * scale
    self_score = jnp.einsum("nkgd,nkd->nkg", grouped, new_keys, preferred_element_type=F32) * scale
    live = jnp.arange(cache_len, dtype=jnp.int32)[None, :] < lengths[:, None]
    scores = jnp.where(live[:, None, None, :], scores, -1e30)
    top = jnp.maximum(jnp.max(scores, axis=3), self_score)
    e = jnp.exp(scores - top[..., None])
    e_self = jnp.exp(self_score - top)
    denom = jnp.sum(e, axis=3) + e_self
    weights = (e / denom[..., None]).astype(BF16)
    w_self = (e_self / denom).astype(BF16)
    context = jnp.einsum("nkgl,nkld->nkgd", weights, cache_values, preferred_element_type=F32)
    context = context + w_self.astype(F32)[..., None] * new_values.astype(F32)[:, :, None, :]
    return context.astype(BF16)


def xor_pairs(k):
    return [(i, i ^ k) for i in range(4)]


SPREAD = [(g * 4 + x, x * 4 + (g ^ x)) for g in range(4) for x in range(4)]
FLIP = [(0, 1), (1, 0)]
CHIP = ("x", "yl")
BLOCK = ("yh", "zh", "zl")
ACROSS = ("yh", "zh", "zl", "yl")


def swap(v, axis):
    return lax.ppermute(v, axis, FLIP)


def cube_of(top, bottom):
    z_top, y_bottom = swap(top, "zl"), swap(bottom, "yl")
    z_bottom, y_top = swap(bottom, "zl"), swap(top, "yl")
    d_bottom, d_top = swap(y_bottom, "zl"), swap(z_top, "yl")
    near, far = [], []
    for pieces, dz, half, v in (
        (near, 0, 0, top),
        (near, 0, 1, bottom),
        (near, 1, 0, z_top),
        (near, 1, 1, z_bottom),
        (far, 0, 1, y_bottom),
        (far, 0, 0, y_top),
        (far, 1, 0, d_top),
        (far, 1, 1, d_bottom),
    ):
        pieces += [(dz, 0, half, v), (dz, 1, half, swap(v, "c"))]
    return near, far


def row_of(w):
    near = {k: lax.ppermute(w, "x", xor_pairs(k)) for k in (1, 3)}
    near[2] = lax.ppermute(w, "x", xor_pairs(2))
    near[0] = w
    pieces = []
    for k in (0, 1, 3, 2):
        pieces += [(k, 0, near[k]), (k, 1, swap(near[k], "c"))]
    return pieces


def matmul_kernel(lhs_pieces, weights, out_shape, place, finish, scalars):
    n = len(weights)

    def body(scalar_ref, *refs):
        lhs_refs, w_refs = refs[: len(lhs_pieces)], refs[len(lhs_pieces) : len(lhs_pieces) + n]
        out_ref, lhs_scr = refs[len(lhs_pieces) + n], refs[len(lhs_pieces) + n + 1]
        bufs, sem = refs[len(lhs_pieces) + n + 2 : -1], refs[-1]
        copies = [pltpu.make_async_copy(w_refs[i], bufs[i], sem.at[i]) for i in range(n)]
        for copy in copies:
            copy.start()
        if place is None:
            lhs_scr = lhs_refs[0]
        else:
            place(scalar_ref, lhs_refs, lhs_scr)
        slots = sorted({slot for _, slot, _ in weights})
        for slot in slots:
            acc = None
            for i, (col, home, w) in enumerate(weights):
                if home != slot:
                    continue
                copies[i].wait()
                if callable(col):
                    at = pl.ds(pl.multiple_of(col(scalar_ref), 128), w.shape[0])
                else:
                    at = slice(col, col + w.shape[0])
                term = jnp.dot(lhs_scr[:, at], bufs[i][...], preferred_element_type=F32)
                acc = term if acc is None else acc + term
            finish(scalar_ref, out_ref, slot, acc.astype(BF16))

    rows = sum(v.shape[0] for v in lhs_pieces)
    depth = lhs_pieces[0].shape[1]
    flops = sum(2 * rows * w.size for _, _, w in weights)
    return pl.pallas_call(
        body,
        out_shape=jax.ShapeDtypeStruct(out_shape, BF16),
        in_specs=[pl.BlockSpec(memory_space=pltpu.SMEM)]
        + [pl.BlockSpec(memory_space=pltpu.VMEM)] * len(lhs_pieces)
        + [pl.BlockSpec(memory_space=pltpu.HBM)] * n,
        out_specs=pl.BlockSpec(memory_space=pltpu.VMEM),
        scratch_shapes=[pltpu.VMEM((rows, depth) if place else (8, 128), BF16)]
        + [pltpu.VMEM(w.shape, BF16) for _, _, w in weights]
        + [pltpu.SemaphoreType.DMA((n,))],
        compiler_params=pltpu.CompilerParams(vmem_limit_bytes=30 << 20),
        cost_estimate=pl.CostEstimate(flops=flops, bytes_accessed=sum(2 * w.size for _, _, w in weights), transcendentals=0),
    )(jnp.stack(scalars).astype(jnp.int32), *lhs_pieces, *[pltpu.with_memory_space_constraint(w, pltpu.HBM) for _, _, w in weights])


def unrelated(pieces, index):
    n = len(pieces)
    out = []
    for j in range(n):
        v = pieces[j]
        for k in range(1, n):
            v = jnp.where(index == k, pieces[j ^ k], v)
        out.append(v)
    return out


def sum_over_x(v):
    return sum((lax.ppermute(v, "x", xor_pairs(k)) for k in (1, 2, 3)), v)


def local(h, attn_gain, ffn_gain, w_query, w_keyval, w_output, cache_keys, cache_values, lengths):
    x_pos = lax.axis_index("x")
    shard = lax.axis_index(("x", "yl", "c"))
    seq_dev, kv_heads, _, head_dim = cache_keys.shape
    tokens, width = h.shape
    quarter = tokens // 4
    model = 16 * width
    wide = 4 * width

    q_cols = w_query.shape[1]
    rows, cols = w_query.shape[0], q_cols + w_keyval.shape[1]
    halves = [jnp.concatenate([w_query[i : i + rows // 2], w_keyval[i : i + rows // 2]], axis=1) for i in (0, rows // 2)]
    w_near, w_far = cube_of(*halves)
    w_out = row_of(w_output)

    sent = h.reshape(4, 4, seq_dev, width).transpose(1, 0, 2, 3).reshape(4, quarter, width)
    got = lax.all_to_all(sent, PAIR, 0, 0, tiled=True)
    core = lax.axis_index("c")
    by_core = h.reshape(8, 2, seq_dev, width)
    mine = lax.dynamic_index_in_dim(by_core, core, 1, keepdims=False).reshape(-1, width)
    other = swap(lax.dynamic_index_in_dim(by_core, 1 - core, 1, keepdims=False), "c").reshape(-1, width)
    home_rows = jnp.concatenate(unrelated([mine, other], core), axis=1)
    resident = got.transpose(1, 0, 2).reshape(quarter, wide).astype(F32)
    squares = sum_over_x(jnp.sum(resident * resident, axis=1))
    inverse = lax.rsqrt(squares / model + EPS)[:, None]
    gain = lax.dynamic_slice_in_dim(attn_gain, x_pos * wide, wide).astype(F32)
    normed = (resident * inverse * gain).astype(BF16)
    z_pos = lax.axis_index("zl")
    normed = jnp.concatenate(unrelated([normed[:, :rows], normed[:, rows:]], z_pos), axis=1)
    normed = lax.ppermute(normed, WIDE, SPREAD)
    slots = [normed] + [lax.ppermute(normed, "x", xor_pairs(k)) for k in (1, 2, 3)]

    order = lax.axis_index("x") ^ lax.axis_index(("yh", "zh"))

    def place_tokens(scalar_ref, lhs_refs, lhs_scr):
        for k, ref in enumerate(lhs_refs):
            at = pl.multiple_of((scalar_ref[0] ^ k) * quarter, quarter)
            lhs_scr[pl.ds(at, quarter), :] = ref[...]

    def put_columns(scalar_ref, out_ref, slot, value):
        out_ref[:, slot * cols : (slot + 1) * cols] = value

    arrived = []
    for pieces in (w_near, w_far):
        partial = matmul_kernel(
            slots,
            [(dz * rows + half * (rows // 2), dc, v) for dz, dc, half, v in pieces],
            (tokens, 2 * cols),
            place_tokens,
            put_columns,
            [order],
        ).reshape(16, seq_dev, 2 * cols)
        arrived.append(lax.all_to_all(partial, WIDE, 0, 0, tiled=True))
    qkv = [jnp.sum(v.reshape(4, 4, seq_dev, 2 * cols).astype(F32), axis=0) for v in arrived]
    pair_pos = lax.axis_index(PAIR)

    def head_block(x, p, start, stop):
        return qkv[p // 2][x, :, (p % 2) * cols + start : (p % 2) * cols + stop]

    q_of = [unrelated([head_block(x, p, 0, q_cols) for p in range(4)], pair_pos) for x in range(4)]
    kv_of = [unrelated([head_block(x, p, q_cols, cols) for p in range(4)], pair_pos) for x in range(4)]
    queries = jnp.concatenate([v for x in q_of for v in x], axis=1).reshape(seq_dev, -1, head_dim)
    keyval = jnp.concatenate([v for x in kv_of for v in x], axis=1).reshape(seq_dev, -1, head_dim)
    own_len = lax.dynamic_slice_in_dim(lengths, shard * seq_dev, seq_dev)
    roped_q = rotate(queries, own_len).astype(BF16)
    new_keys = rotate(keyval[:, :kv_heads], own_len).astype(BF16)
    new_values = keyval[:, kv_heads:].astype(BF16)
    per_kv = roped_q.shape[1] // kv_heads
    grouped = roped_q.reshape(seq_dev, kv_heads, per_kv, head_dim)
    context = attend(grouped, new_keys, new_values, cache_keys, cache_values, own_len)

    context = context.reshape(seq_dev, 4, 2, 2 * width).transpose(2, 0, 1, 3).reshape(1, 2, seq_dev, 2 * wide)
    context = jnp.broadcast_to(context, (8, 2, seq_dev, 2 * wide)).reshape(16, seq_dev, 2 * wide)
    context = lax.all_to_all(context, ACROSS, 0, 0, tiled=True).reshape(tokens, 2 * wide)
    out_cols = w_output.shape[1]
    chip = lax.axis_index(CHIP)
    part = 2 * seq_dev

    def column_of(dx, dc):
        return lambda scalar_ref: ((scalar_ref[0] ^ dx) * 2 + (scalar_ref[1] ^ dc)) * width

    def put_blocks(scalar_ref, out_ref, slot, value):
        for g in range(8):
            out_ref[g] = value[g * part : (g + 1) * part]

    out = matmul_kernel(
        [context],
        [(column_of(dx, dc), 0, v) for dx, dc, v in w_out],
        (8, part, out_cols),
        None,
        put_blocks,
        [x_pos, core],
    )
    out = lax.all_to_all(out, BLOCK, 0, 0, tiled=True)
    out = lax.all_to_all(out, CHIP, 0, 0, tiled=True)
    summed = jnp.sum(out.reshape(4, 2, part, out_cols).astype(F32), axis=1).reshape(tokens // 2, out_cols)
    stream = home_rows.astype(F32) + summed
    squares_two = jnp.sum(stream * stream, axis=1)
    squares_two = lax.all_to_all(jnp.broadcast_to(squares_two[None], (8, tokens // 2)), CHIP, 0, 0, tiled=True)
    inverse_two = lax.rsqrt(jnp.sum(squares_two, axis=0) / model + EPS)[:, None]
    gain_two = lax.dynamic_slice_in_dim(ffn_gain, chip * out_cols, out_cols).astype(F32)
    ffn_input = (stream * inverse_two * gain_two).astype(BF16)
    both = jnp.stack([summed.astype(BF16), ffn_input]).reshape(2, tokens // 2, 2, width)
    keep = lax.dynamic_index_in_dim(both, core, 2, keepdims=False)
    came = swap(lax.dynamic_index_in_dim(both, 1 - core, 2, keepdims=False), "c")
    keep, came = keep.reshape(2, 8, seq_dev, width), came.reshape(2, 8, seq_dev, width)
    return tuple(
        jnp.stack(unrelated([keep[i], came[i]], core), axis=1).reshape(tokens, width) for i in range(2)
    )


def solution(mesh):
    fine = Mesh(mesh.devices.reshape(2, 2, 2, 4, 2, 2), ("yh", "zh", "zl", "x", "yl", "c"))
    group = ("yh", "zh", "zl")
    shard = ("x", "yl", "c")
    placed = (
        P(group, shard),
        P(),
        P(),
        P(group, shard),
        P(group, shard),
        P(shard, group),
        P(group + shard, None, None, None),
        P(group + shard, None, None, None),
        P(group),
    )
    return jax.shard_map(
        local,
        mesh=fine,
        in_specs=placed,
        out_specs=(P(group, shard), P(group, shard)),
        check_vma=False,
    )
```

```python
import jax
import jax.numpy as jnp
from jax import lax
from jax.experimental import pallas as pl
from jax.experimental.pallas import tpu as pltpu
from jax.sharding import Mesh, PartitionSpec as P

EPS = 1e-05
ROPE_BASE = 500000.0
F32 = jnp.float32
BF16 = jnp.bfloat16


PAIR = ("yl", "c")
WIDE = ("yh", "zh", "x")


def rotate(v, position):
    half = v.shape[-1] // 2
    freq = ROPE_BASE ** (-2.0 * jnp.arange(half, dtype=F32) / v.shape[-1])
    angles = position.astype(F32)[:, None] * freq[None, :]
    cos = jnp.cos(angles)[:, None, :]
    sin = jnp.sin(angles)[:, None, :]
    low, high = v[..., :half], v[..., half:]
    return jnp.concatenate([low * cos - high * sin, high * cos + low * sin], axis=-1)


def attend(grouped, new_keys, new_values, cache_keys, cache_values, lengths):
    _, _, cache_len, head_dim = cache_keys.shape
    scale = head_dim ** (-0.5)
    scores = jnp.einsum("nkgd,nkld->nkgl", grouped, cache_keys, preferred_element_type=F32) * scale
    self_score = jnp.einsum("nkgd,nkd->nkg", grouped, new_keys, preferred_element_type=F32) * scale
    live = jnp.arange(cache_len, dtype=jnp.int32)[None, :] < lengths[:, None]
    scores = jnp.where(live[:, None, None, :], scores, -1e30)
    top = jnp.maximum(jnp.max(scores, axis=3), self_score)
    e = jnp.exp(scores - top[..., None])
    e_self = jnp.exp(self_score - top)
    denom = jnp.sum(e, axis=3) + e_self
    weights = (e / denom[..., None]).astype(BF16)
    w_self = (e_self / denom).astype(BF16)
    context = jnp.einsum("nkgl,nkld->nkgd", weights, cache_values, preferred_element_type=F32)
    context = context + w_self.astype(F32)[..., None] * new_values.astype(F32)[:, :, None, :]
    return context.astype(BF16)


def xor_pairs(k):
    return [(i, i ^ k) for i in range(4)]


SPREAD = [(g * 4 + x, x * 4 + (g ^ x)) for g in range(4) for x in range(4)]
FLIP = [(0, 1), (1, 0)]
CHIP = ("x", "yl")
BLOCK = ("yh", "zh", "zl")
ACROSS = ("yh", "zh", "zl", "yl")


def swap(v, axis):
    return lax.ppermute(v, axis, FLIP)


def cube_of(top, bottom):
    z_top, y_bottom = swap(top, "zl"), swap(bottom, "yl")
    z_bottom, y_top = swap(bottom, "zl"), swap(top, "yl")
    d_bottom, d_top = swap(y_bottom, "zl"), swap(z_top, "yl")
    near, far = [], []
    for pieces, dz, half, v in (
        (near, 0, 0, top),
        (near, 0, 1, bottom),
        (near, 1, 0, z_top),
        (near, 1, 1, z_bottom),
        (far, 0, 1, y_bottom),
        (far, 0, 0, y_top),
        (far, 1, 0, d_top),
        (far, 1, 1, d_bottom),
    ):
        pieces += [(dz, 0, half, v), (dz, 1, half, swap(v, "c"))]
    return near, far


def row_of(w):
    near = {k: lax.ppermute(w, "x", xor_pairs(k)) for k in (1, 3)}
    near[2] = lax.ppermute(w, "x", xor_pairs(2))
    near[0] = w
    pieces = []
    for k in (0, 1, 3, 2):
        pieces += [(k, 0, near[k]), (k, 1, swap(near[k], "c"))]
    return pieces


def matmul_kernel(lhs_pieces, weights, out_shape, place, finish, scalars):
    n = len(weights)

    def body(scalar_ref, *refs):
        lhs_refs, w_refs = refs[: len(lhs_pieces)], refs[len(lhs_pieces) : len(lhs_pieces) + n]
        out_ref, lhs_scr = refs[len(lhs_pieces) + n], refs[len(lhs_pieces) + n + 1]
        bufs, sem = refs[len(lhs_pieces) + n + 2 : -1], refs[-1]
        copies = [pltpu.make_async_copy(w_refs[i], bufs[i], sem.at[i]) for i in range(n)]
        for copy in copies:
            copy.start()
        if place is None:
            lhs_scr = lhs_refs[0]
        else:
            place(scalar_ref, lhs_refs, lhs_scr)
        slots = sorted({slot for _, slot, _ in weights})
        for slot in slots:
            acc = None
            for i, (col, home, w) in enumerate(weights):
                if home != slot:
                    continue
                copies[i].wait()
                if callable(col):
                    at = pl.ds(pl.multiple_of(col(scalar_ref), 128), w.shape[0])
                else:
                    at = slice(col, col + w.shape[0])
                term = jnp.dot(lhs_scr[:, at], bufs[i][...], preferred_element_type=F32)
                acc = term if acc is None else acc + term
            finish(scalar_ref, out_ref, slot, acc.astype(BF16))

    rows = sum(v.shape[0] for v in lhs_pieces)
    depth = lhs_pieces[0].shape[1]
    flops = sum(2 * rows * w.size for _, _, w in weights)
    return pl.pallas_call(
        body,
        out_shape=jax.ShapeDtypeStruct(out_shape, BF16),
        in_specs=[pl.BlockSpec(memory_space=pltpu.SMEM)]
        + [pl.BlockSpec(memory_space=pltpu.VMEM)] * len(lhs_pieces)
        + [pl.BlockSpec(memory_space=pltpu.HBM)] * n,
        out_specs=pl.BlockSpec(memory_space=pltpu.VMEM),
        scratch_shapes=[pltpu.VMEM((rows, depth) if place else (8, 128), BF16)]
        + [pltpu.VMEM(w.shape, BF16) for _, _, w in weights]
        + [pltpu.SemaphoreType.DMA((n,))],
        compiler_params=pltpu.CompilerParams(vmem_limit_bytes=30 << 20),
        cost_estimate=pl.CostEstimate(flops=flops, bytes_accessed=sum(2 * w.size for _, _, w in weights), transcendentals=0),
    )(jnp.stack(scalars).astype(jnp.int32), *lhs_pieces, *[pltpu.with_memory_space_constraint(w, pltpu.HBM) for _, _, w in weights])


def unrelated(pieces, index):
    n = len(pieces)
    out = []
    for j in range(n):
        v = pieces[j]
        for k in range(1, n):
            v = jnp.where(index == k, pieces[j ^ k], v)
        out.append(v)
    return out


def sum_over_x(v):
    return sum((lax.ppermute(v, "x", xor_pairs(k)) for k in (1, 2, 3)), v)


def local(h, attn_gain, ffn_gain, w_query, w_keyval, w_output, cache_keys, cache_values, lengths):
    x_pos = lax.axis_index("x")
    shard = lax.axis_index(("x", "yl", "c"))
    seq_dev, kv_heads, _, head_dim = cache_keys.shape
    tokens, width = h.shape
    quarter = tokens // 4
    model = 16 * width
    wide = 4 * width

    q_cols = w_query.shape[1]
    rows, cols = w_query.shape[0], q_cols + w_keyval.shape[1]
    halves = [jnp.concatenate([w_query[i : i + rows // 2], w_keyval[i : i + rows // 2]], axis=1) for i in (0, rows // 2)]
    w_near, w_far = cube_of(*halves)
    w_out = row_of(w_output)

    sent = h.reshape(4, 4, seq_dev, width).transpose(1, 0, 2, 3).reshape(4, quarter, width)
    got = lax.all_to_all(sent, PAIR, 0, 0, tiled=True)
    core = lax.axis_index("c")
    by_core = h.reshape(8, 2, seq_dev, width)
    mine = lax.dynamic_index_in_dim(by_core, core, 1, keepdims=False).reshape(-1, width)
    other = swap(lax.dynamic_index_in_dim(by_core, 1 - core, 1, keepdims=False), "c").reshape(-1, width)
    home_rows = jnp.concatenate(unrelated([mine, other], core), axis=1)
    resident = got.transpose(1, 0, 2).reshape(quarter, wide)
    squares = sum_over_x(jnp.sum(jnp.square(resident.astype(F32)), axis=1))
    inverse = lax.rsqrt(squares / model + EPS)
    z_pos, plane = lax.axis_index("zl"), lax.axis_index(("yh", "zh"))
    raw = jnp.concatenate(unrelated([resident[:, :rows], resident[:, rows:]], z_pos), axis=1)
    raw = lax.ppermute(raw, WIDE, SPREAD)
    inverse = lax.ppermute(inverse, WIDE, SPREAD)[:, None]
    gain = lax.dynamic_slice_in_dim(attn_gain, plane * wide, wide).astype(F32)
    gain = jnp.concatenate(unrelated([gain[:rows], gain[rows:]], z_pos))
    normed = (raw.astype(F32) * inverse * gain).astype(BF16)
    slots = [normed] + [lax.ppermute(normed, "x", xor_pairs(k)) for k in (1, 2, 3)]

    order = lax.axis_index("x") ^ lax.axis_index(("yh", "zh"))

    def place_tokens(scalar_ref, lhs_refs, lhs_scr):
        for k, ref in enumerate(lhs_refs):
            at = pl.multiple_of((scalar_ref[0] ^ k) * quarter, quarter)
            lhs_scr[pl.ds(at, quarter), :] = ref[...]

    def put_columns(scalar_ref, out_ref, slot, value):
        out_ref[:, slot * cols : (slot + 1) * cols] = value

    arrived = []
    for pieces in (w_near, w_far):
        partial = matmul_kernel(
            slots,
            [(dz * rows + half * (rows // 2), dc, v) for dz, dc, half, v in pieces],
            (tokens, 2 * cols),
            place_tokens,
            put_columns,
            [order],
        ).reshape(16, seq_dev, 2 * cols)
        arrived.append(lax.all_to_all(partial, WIDE, 0, 0, tiled=True))
    qkv = [jnp.sum(v.reshape(4, 4, seq_dev, 2 * cols).astype(F32), axis=0) for v in arrived]
    pair_pos = lax.axis_index(PAIR)

    def head_block(x, p, start, stop):
        return qkv[p // 2][x, :, (p % 2) * cols + start : (p % 2) * cols + stop]

    q_of = [unrelated([head_block(x, p, 0, q_cols) for p in range(4)], pair_pos) for x in range(4)]
    kv_of = [unrelated([head_block(x, p, q_cols, cols) for p in range(4)], pair_pos) for x in range(4)]
    queries = jnp.concatenate([v for x in q_of for v in x], axis=1).reshape(seq_dev, -1, head_dim)
    keyval = jnp.concatenate([v for x in kv_of for v in x], axis=1).reshape(seq_dev, -1, head_dim)
    own_len = lax.dynamic_slice_in_dim(lengths, shard * seq_dev, seq_dev)
    roped_q = rotate(queries, own_len).astype(BF16)
    new_keys = rotate(keyval[:, :kv_heads], own_len).astype(BF16)
    new_values = keyval[:, kv_heads:].astype(BF16)
    per_kv = roped_q.shape[1] // kv_heads
    grouped = roped_q.reshape(seq_dev, kv_heads, per_kv, head_dim)
    context = attend(grouped, new_keys, new_values, cache_keys, cache_values, own_len)

    context = context.reshape(seq_dev, 4, 2, 2 * width).transpose(2, 0, 1, 3).reshape(1, 2, seq_dev, 2 * wide)
    context = jnp.broadcast_to(context, (8, 2, seq_dev, 2 * wide)).reshape(16, seq_dev, 2 * wide)
    context = lax.all_to_all(context, ACROSS, 0, 0, tiled=True).reshape(tokens, 2 * wide)
    out_cols = w_output.shape[1]
    chip = lax.axis_index(CHIP)
    part = 2 * seq_dev

    def column_of(dx, dc):
        return lambda scalar_ref: ((scalar_ref[0] ^ dx) * 2 + (scalar_ref[1] ^ dc)) * width

    def put_blocks(scalar_ref, out_ref, slot, value):
        for g in range(8):
            out_ref[g] = value[g * part : (g + 1) * part]

    out = matmul_kernel(
        [context],
        [(column_of(dx, dc), 0, v) for dx, dc, v in w_out],
        (8, part, out_cols),
        None,
        put_blocks,
        [x_pos, core],
    )
    out = lax.all_to_all(out, BLOCK, 0, 0, tiled=True)
    out = lax.all_to_all(out, CHIP, 0, 0, tiled=True)
    summed = jnp.sum(out.reshape(4, 2, part, out_cols).astype(F32), axis=1).reshape(tokens // 2, out_cols)
    stream = home_rows.astype(F32) + summed
    squares_two = jnp.sum(stream * stream, axis=1)
    squares_two = lax.all_to_all(jnp.broadcast_to(squares_two[None], (8, tokens // 2)), CHIP, 0, 0, tiled=True)
    inverse_two = lax.rsqrt(jnp.sum(squares_two, axis=0) / model + EPS)[:, None]
    gain_two = lax.dynamic_slice_in_dim(ffn_gain, chip * out_cols, out_cols).astype(F32)
    ffn_input = (stream * inverse_two * gain_two).astype(BF16)
    both = jnp.stack([summed.astype(BF16), ffn_input]).reshape(2, tokens // 2, 2, width)
    keep = lax.dynamic_index_in_dim(both, core, 2, keepdims=False)
    came = swap(lax.dynamic_index_in_dim(both, 1 - core, 2, keepdims=False), "c")
    keep, came = keep.reshape(2, 8, seq_dev, width), came.reshape(2, 8, seq_dev, width)
    return tuple(
        jnp.stack(unrelated([keep[i], came[i]], core), axis=1).reshape(tokens, width) for i in range(2)
    )


def solution(mesh):
    fine = Mesh(mesh.devices.reshape(2, 2, 2, 4, 2, 2), ("yh", "zh", "zl", "x", "yl", "c"))
    group = ("yh", "zh", "zl")
    shard = ("x", "yl", "c")
    placed = (
        P(group, shard),
        P(),
        P(),
        P(group, shard),
        P(group, shard),
        P(shard, group),
        P(group + shard, None, None, None),
        P(group + shard, None, None, None),
        P(group),
    )
    return jax.shard_map(
        local,
        mesh=fine,
        in_specs=placed,
        out_specs=(P(group, shard), P(group, shard)),
        check_vma=False,
    )
```
